512 devices in a mesh: sp: 64 (over z, y_hi, core), dp: 8 (over y_lo, x).
Axes of the slice: x: 4, y: 8 (y_hi: 4, y_lo: 2; y = y_hi * 2 + y_lo), z: 8, core: 2. Of those that a mesh axis runs over, the one named last changes fastest.
Arguments:
- query_proj: bfloat16 [65536, 8192], P(('dp', 'sp')), parts along dimension 0, may hold values from -64 to 64
- key_projection: bfloat16 [65536, 1024], P(('dp', 'sp')), parts along dimension 0, may hold values from -64 to 64
- value_projection: bfloat16 [65536, 1024], P(('dp', 'sp')), parts along dimension 0, may hold values from -12 to 12
- query_gain: float32 [128], replicated, may hold values from 1 to 5
- key_norm_gain: float32 [128], replicated, may hold values from 1 to 5
- positions: int32 [65536], P(('dp', 'sp')), parts along dimension 0, may hold values from 0 to 5118, as said below
- doc_start: int32 [65536], P(('dp', 'sp')), parts along dimension 0, may hold values from 0 to 8191, as said below
Outputs:
- attention: bfloat16 [65536, 8192], P(('dp', 'sp')), parts along dimension 0
The draws below stay inside these ranges and needn't reach their ends.
There are 8 independent parts, one for each index of `dp`. The reference program is written for one: setup_inputs(seed, part) draws one part's arguments, and reference() takes and returns one part's arrays. A program takes and returns all parts, laid end to end along the dimension named above; an argument that names none is the same for every part. Nothing has to cross between parts.
Inputs may be any that keep to these rules, and one draw needn't show every extreme that they name: doc_start[i] is the index of the first token of token i's document: it never falls, doc_start[i] <= i < doc_start[i] + 1024, some document has exactly 1024 tokens, and every document but the last has 128 tokens or more. `positions`: within one document the position rises by one from each token to the next.
All inputs are finite; a program needn't handle non-finite values.
Results may differ from the reference program's by a relative error of at most 0.0039.
The reference program's roundings to bfloat16 on the way count: a program that leaves them out, or rounds other values in their place, can miss the bound.
Values may be sent and summed in bfloat16 or wider, within the bound.
A program may use at most 64 MiB of HBM per device.

```python
import jax
import jax.numpy as jnp
from jax import lax

QUERY_HEADS = 64
KEY_VALUE_HEADS = 8
HEAD_SIZE = 128
DOC_MAX = 1024
PACK_TOKENS = 8192


def doc_layout(key):
    rotary_base = jax.random.fold_in(key, 11)
    shortest = DOC_MAX // 8
    count = PACK_TOKENS // shortest + 1
    lengths = jax.random.randint(jax.random.fold_in(rotary_base, 1), (count,), shortest, DOC_MAX + 1, dtype=jnp.int32)
    forced = jax.random.randint(jax.random.fold_in(rotary_base, 2), (), 0, 2, dtype=jnp.int32)
    lengths = jnp.where(jnp.arange(count, dtype=jnp.int32) == forced, DOC_MAX, lengths).astype(jnp.int32)
    starts = (jnp.cumsum(lengths) - lengths).astype(jnp.int32)
    token_index = jnp.arange(PACK_TOKENS, dtype=jnp.int32)
    doc_index = jnp.sum((starts[None, :] <= token_index[:, None]).astype(jnp.int32), axis=1) - 1
    doc_first = starts[doc_index]
    offsets = jax.random.randint(jax.random.fold_in(rotary_base, 3), (count,), 0, 4 * DOC_MAX, dtype=jnp.int32)
    positions = offsets[doc_index] + token_index - doc_first
    return (doc_first.astype(jnp.int32), positions.astype(jnp.int32))


def qk_fields(key):
    rotary_base = jax.random.fold_in(key, 23)
    q_vals = jax.random.normal(jax.random.fold_in(rotary_base, 1), (PACK_TOKENS, QUERY_HEADS, HEAD_SIZE), jnp.float32)
    key_values_local = jax.random.normal(jax.random.fold_in(rotary_base, 2), (PACK_TOKENS, KEY_VALUE_HEADS, HEAD_SIZE), jnp.float32)
    q_vals = jnp.clip(q_vals, -64.0, 64.0).reshape(PACK_TOKENS, QUERY_HEADS * HEAD_SIZE)
    key_values_local = jnp.clip(key_values_local, -64.0, 64.0).reshape(PACK_TOKENS, KEY_VALUE_HEADS * HEAD_SIZE)
    return (q_vals, key_values_local)


def draw_query_proj(key, part):
    return qk_fields(key)[0].astype(jnp.bfloat16)


def draw_key_projection(key, part):
    return qk_fields(key)[1].astype(jnp.bfloat16)


def draw_query_gain(key, part):
    sub_key = jax.random.fold_in(key, 31)
    return jax.random.uniform(sub_key, (HEAD_SIZE,), jnp.float32, 1.0, 2.0)


def draw_key_norm_gain(key, part):
    sub_key = jax.random.fold_in(key, 37)
    return jax.random.uniform(sub_key, (HEAD_SIZE,), jnp.float32, 1.0, 2.0)


def draw_positions(key, part):
    return doc_layout(key)[1]


def draw_doc_start(key, part):
    return doc_layout(key)[0]


def block_levels(rng, dims, pieces, smallest, largest):
    loudness, own = 1.0, jax.random.fold_in(rng, 6)
    for axis_at, blocks in pieces:
        steps = jnp.exp(jax.random.uniform(jax.random.fold_in(own, axis_at), (blocks,), jnp.float32, smallest / len(pieces), largest / len(pieces)))
        loudness = loudness * jnp.repeat(steps, dims[axis_at] // blocks).reshape([-1 if axis == axis_at else 1 for axis in range(len(dims))])
    return loudness


def normal_values(own_key, extent, spread, reach, split=(), held_as=jnp.bfloat16):
    drawn = spread * jax.random.normal(own_key, extent, jnp.float32)
    if split:
        drawn = drawn * block_levels(own_key, extent, split, -0.22, 0.18)
    return jnp.clip(drawn, -reach, reach).astype(held_as)


def setup_inputs(seed: int = 0, part: int = 0) -> dict:
    key_of = jax.random.split(jax.random.key(seed), 8)
    own_keys = jax.random.split(jax.random.fold_in(key_of[7], part), 8)
    return {
        "query_proj": draw_query_proj(jax.random.fold_in(jax.random.fold_in(key_of[7], part), 71), part),
        "key_projection": draw_key_projection(jax.random.fold_in(jax.random.fold_in(key_of[7], part), 71), part),
        "value_projection": normal_values(own_keys[2], (PACK_TOKENS, KEY_VALUE_HEADS * HEAD_SIZE), 2.0, 12.0, ((0, 64),)),
        "query_gain": draw_query_gain(jax.random.fold_in(key_of[7], 71), part),
        "key_norm_gain": draw_key_norm_gain(jax.random.fold_in(key_of[7], 71), part),
        "positions": draw_positions(jax.random.fold_in(jax.random.fold_in(key_of[7], part), 71), part),
        "doc_start": draw_doc_start(jax.random.fold_in(jax.random.fold_in(key_of[7], part), 71), part),
    }


ROPE_BASE = 1000000.0
NORM_EPS = 1e-06

def rotary_tables(positions):
    half_dim = HEAD_SIZE // 2
    inv_freq = ROPE_BASE ** (-(jnp.arange(half_dim, dtype=jnp.float32) * 2.0 / HEAD_SIZE))
    angle = positions.astype(jnp.float32)[:, None] * inv_freq[None, :]
    return (jnp.cos(angle), jnp.sin(angle))

def normalize_and_rotate(heads_in, gain, cosine_table, sine_table):
    upcast = heads_in.astype(jnp.float32)
    mean_square = lax.optimization_barrier(jnp.mean(upcast * upcast, axis=-1, keepdims=True))
    normed = upcast * lax.rsqrt(mean_square + NORM_EPS) * gain
    half_dim = normed.shape[-1] // 2
    first_half = normed[..., :half_dim]
    second_half = normed[..., half_dim:]
    cos_rows = cosine_table[:, None, :]
    sin_rows = sine_table[:, None, :]
    rotated = jnp.concatenate([first_half * cos_rows - second_half * sin_rows, second_half * cos_rows + first_half * sin_rows], axis=-1)
    return rotated.astype(jnp.bfloat16)

def attend(q_head, k_head, v_head, starts):
    rows_all = q_head.shape[0]
    block_rows = min(512, rows_all)
    key_window = DOC_MAX + block_rows
    zero_rows = jnp.zeros((DOC_MAX, q_head.shape[1]), q_head.dtype)
    k_padded = jnp.concatenate([zero_rows, k_head], axis=0)
    v_padded = jnp.concatenate([zero_rows, v_head], axis=0)
    scale = q_head.shape[1] ** (-0.5)

    def one_block(block_index):
        block_start = (block_index * block_rows).astype(jnp.int32)
        query_block = lax.dynamic_slice_in_dim(q_head, block_start, block_rows, 0)
        key_block = lax.dynamic_slice_in_dim(k_padded, block_start, key_window, 0)
        value_block = lax.dynamic_slice_in_dim(v_padded, block_start, key_window, 0)
        doc_first = lax.dynamic_slice_in_dim(starts, block_start, block_rows, 0)
        row_index = block_start + jnp.arange(block_rows, dtype=jnp.int32)
        key_index = block_start - DOC_MAX + jnp.arange(key_window, dtype=jnp.int32)
        visible = (key_index[None, :] >= doc_first[:, None]) & (key_index[None, :] <= row_index[:, None])
        scores = jnp.dot(query_block, key_block.T, preferred_element_type=jnp.float32) * scale
        scores = jnp.where(visible, scores, -jnp.inf)
        row_max = lax.optimization_barrier(jnp.max(scores, axis=1, keepdims=True))
        exp_scores = jnp.exp(scores - row_max)
        row_total = lax.optimization_barrier(jnp.sum(exp_scores, axis=1, keepdims=True))
        weights = exp_scores.astype(jnp.bfloat16)
        mixed_out = jnp.dot(weights, value_block, preferred_element_type=jnp.float32) / row_total
        return mixed_out.astype(jnp.bfloat16)
    blocks = lax.map(one_block, jnp.arange(rows_all // block_rows, dtype=jnp.int32))
    return blocks.reshape(rows_all, q_head.shape[1])

def reference(query_proj, key_projection, value_projection, query_gain, key_norm_gain, positions, doc_start):
    cosine_table, sine_table = rotary_tables(positions)
    q_rope = normalize_and_rotate(query_proj.reshape(PACK_TOKENS, QUERY_HEADS, HEAD_SIZE), query_gain, cosine_table, sine_table)
    key_rotated = normalize_and_rotate(key_projection.reshape(PACK_TOKENS, KEY_VALUE_HEADS, HEAD_SIZE), key_norm_gain, cosine_table, sine_table)
    value_head_split = value_projection.reshape(PACK_TOKENS, KEY_VALUE_HEADS, HEAD_SIZE)
    head_copies = QUERY_HEADS // KEY_VALUE_HEADS
    q_major = jnp.transpose(q_rope, (1, 0, 2))
    k_major = jnp.repeat(jnp.transpose(key_rotated, (1, 0, 2)), head_copies, axis=0)
    v_major = jnp.repeat(jnp.transpose(value_head_split, (1, 0, 2)), head_copies, axis=0)

    def one_head(operands):
        return attend(operands[0], operands[1], operands[2], doc_start)
    per_head = lax.map(one_head, (q_major, k_major, v_major))
    return jnp.transpose(per_head, (1, 0, 2)).reshape(PACK_TOKENS, QUERY_HEADS * HEAD_SIZE)
```

```python
import functools

import jax
import jax.numpy as jnp
import numpy as np
from jax import lax
from jax.experimental import pallas as pl
from jax.experimental.pallas import tpu as pltpu
from jax.sharding import PartitionSpec as P

QUERY_HEADS = 64
GROUPS = 8
HEAD = 128
COPIES = QUERY_HEADS // GROUPS
ROWS = 128
ROPE_BASE = 1000000.0
NORM_EPS = 1e-06
COLS = 4

OWN, PREV, WEST, EAST, OPP, X_P, WEST_P, EAST_P, OPP_P, HOLD_E, HOLD_K = range(11)
WINDOW = 9
SLOTS = 11
UP, TO_E, TO_W, REL_E, REL_W, LIFT_E, LIFT_K, D_X, D_W, D_E, D_O = range(11)
KINDS = 11
MESH = pl.DeviceIdType.MESH
HEADS_AT_ONCE = 2


def kernel(
    nz,
    q_hbm,
    k_ref,
    v_hbm,
    q_gain_ref,
    k_gain_ref,
    pos_ref,
    doc_ref,
    freq_ref,
    out_hbm,
    kv,
    q_in,
    out_buf,
    bias,
    cos_tab,
    sin_tab,
    send_sem,
    recv_sem,
    q_sem,
    v_sem,
    out_sem,
):
    me = lax.axis_index("sp")
    core = lax.rem(me, 2)
    y = lax.rem(lax.div(me, 2), COLS)
    z = lax.div(me, 2 * COLS)

    def device(z_at, y_at, core_at):
        return (z_at * COLS + y_at) * 2 + core_at

    east_y = lax.rem(y + 1, COLS)
    west_y = lax.rem(y + COLS - 1, COLS)
    opp_y = lax.rem(y + 2, COLS)
    east = device(z, east_y, core)
    west = device(z, west_y, core)
    up = device(lax.rem(z + 1, nz), y, core)
    down = device(lax.rem(z + nz - 1, nz), y, core)
    partner = device(z, y, 1 - core)

    src_e = jnp.where(y == 3, PREV, OWN)
    src_w = jnp.where(y >= 2, PREV, OWN)
    dst_w = jnp.where(y == 1, HOLD_E, EAST)
    dst_rel_e = jnp.where(y == 3, HOLD_K, OPP)
    src_rel_w = jnp.where(y == 0, HOLD_E, EAST)
    src_x = jnp.where(core == 0, OWN, PREV)

    def copy(r, kind):
        src, dst, target = {
            UP: (kv.at[r, OWN], kv.at[r, PREV], up),
            TO_E: (kv.at[r, src_e], kv.at[r, WEST], east),
            TO_W: (kv.at[r, src_w], kv.at[r, dst_w], west),
            REL_E: (kv.at[r, WEST, 0], kv.at[r, dst_rel_e, 0], east),
            REL_W: (kv.at[r, src_rel_w, 1], kv.at[r, OPP, 1], west),
            LIFT_E: (kv.at[r, HOLD_E], kv.at[r, EAST], up),
            LIFT_K: (kv.at[r, HOLD_K, 0], kv.at[r, OPP, 0], up),
            D_X: (kv.at[r, src_x], kv.at[r, X_P], partner),
            D_W: (kv.at[r, WEST], kv.at[r, WEST_P], partner),
            D_E: (kv.at[r, EAST], kv.at[r, EAST_P], partner),
            D_O: (kv.at[r, OPP], kv.at[r, OPP_P], partner),
        }[kind]
        return pltpu.make_async_remote_copy(
            src_ref=src,
            dst_ref=dst,
            send_sem=send_sem.at[r, kind],
            recv_sem=recv_sem.at[r, kind],
            device_id={"sp": target},
            device_id_type=MESH,
        )

    def v_copy(g):
        return pltpu.make_async_copy(
            v_hbm.at[:, pl.ds(g * HEAD, HEAD)], kv.at[g, OWN, 1], v_sem.at[g]
        )

    def q_copy(g):
        return pltpu.make_async_copy(
            q_hbm.at[:, pl.ds(g * COPIES * HEAD, COPIES * HEAD)], q_in.at[g], q_sem.at[g]
        )

    def out_copy(g):
        return pltpu.make_async_copy(
            out_buf.at[g],
            out_hbm.at[:, pl.ds(pl.multiple_of(g * COPIES * HEAD, COPIES * HEAD), COPIES * HEAD)],
            out_sem.at[g],
        )

    barrier = pltpu.get_barrier_semaphore()
    for target in (east, west, up, down, partner):
        pl.semaphore_signal(barrier, inc=1, device_id={"sp": target}, device_id_type=MESH)
    for g in range(GROUPS):
        v_copy(g).start()
    for g in range(GROUPS):
        q_copy(g).start()

    def column(row):
        return jnp.transpose(jnp.broadcast_to(row.astype(jnp.float32), (ROWS, ROWS)))

    angle = column(pos_ref[...]) * freq_ref[...]
    lane = lax.broadcasted_iota(jnp.int32, (ROWS, HEAD), 1)
    cos_tab[...] = jnp.cos(angle)
    sine = jnp.sin(angle)
    sin_tab[...] = jnp.where(lane < HEAD // 2, -sine, sine)

    def norm_rope(block, gain):
        x = block.astype(jnp.float32)
        mean_square = jnp.mean(x * x, axis=1, keepdims=True)
        normed = x * lax.rsqrt(mean_square + NORM_EPS) * gain
        turned = pltpu.roll(normed, HEAD // 2, 1)
        return (normed * cos_tab[...] + turned * sin_tab[...]).astype(jnp.bfloat16)

    for g in range(GROUPS):
        kv[g, OWN, 0] = norm_rope(k_ref[:, g * HEAD : (g + 1) * HEAD], k_gain_ref[...])
    for g in range(GROUPS):
        v_copy(g).wait()
    pl.semaphore_wait(barrier, 5)

    @pl.loop(0, GROUPS)
    def _(r):
        copy(r, UP).start()

    def spread(r):
        copy(r, UP).wait_recv()
        copy(r, TO_E).start()
        copy(r, TO_W).start()
        copy(r, D_X).start()

    def relay(r):
        copy(r, TO_E).wait_recv()
        copy(r, REL_E).start()
        copy(r, D_W).start()
        copy(r, TO_W).wait_recv()
        copy(r, REL_W).start()

        @pl.when(y == 0)
        def _():
            copy(r, LIFT_E).start()

        @pl.when(y != 0)
        def _():
            copy(r, D_E).start()

    def gather(r):
        copy(r, REL_E).wait_recv()

        @pl.when(y == 0)
        def _():
            copy(r, LIFT_K).start()
            copy(r, LIFT_E).wait_recv()
            copy(r, D_E).start()
            copy(r, LIFT_K).wait_recv()

        copy(r, REL_W).wait_recv()
        copy(r, D_O).start()

    row_first = me * ROWS
    tokens_before = column(doc_ref[...])
    row_at = (row_first + lax.broadcasted_iota(jnp.int32, (ROWS, ROWS), 0)).astype(jnp.float32)

    def base_of(slot):
        if slot == OWN:
            return me * ROWS
        if slot == X_P:
            of_prev = device(z - 1, y, 1 - core)
            return jnp.where(core == 1, me - 1, of_prev) * ROWS
        col = {PREV: y, WEST: west_y, EAST: east_y, OPP: opp_y}[
            slot if slot < X_P else slot - X_P + PREV
        ]
        at = core if slot < X_P else 1 - core
        return device(jnp.where(col >= y, z - 1, z), col, at) * ROWS

    def attend(r):
        for kind in (D_X, D_W, D_E, D_O):
            copy(r, kind).wait_recv()
        keys = kv[r, pl.ds(0, WINDOW), 0].reshape(WINDOW * ROWS, HEAD)
        values = kv[r, pl.ds(0, WINDOW), 1].reshape(WINDOW * ROWS, HEAD)
        wide = HEADS_AT_ONCE * HEAD

        @pl.loop(0, COPIES // HEADS_AT_ONCE)
        def _(step):
            at = pl.multiple_of(step * wide, wide)
            block = q_in[r, :, pl.ds(at, wide)]
            for h in range(HEADS_AT_ONCE):
                q = norm_rope(block[:, h * HEAD : (h + 1) * HEAD], q_gain_ref[...])
                scores = lax.dot_general(
                    q, keys, (((1,), (1,)), ((), ())), preferred_element_type=jnp.float32
                )
                scores = scores * HEAD ** (-0.5) + bias[...]
                top = jnp.max(scores, axis=1, keepdims=True)
                exp_scores = jnp.exp(scores - top)
                total = jnp.sum(exp_scores, axis=1, keepdims=True)
                mixed = jnp.dot(
                    exp_scores.astype(jnp.bfloat16), values, preferred_element_type=jnp.float32
                )
                out_buf[r, :, pl.ds(pl.multiple_of(at + h * HEAD, HEAD), HEAD)] = (
                    mixed / total
                ).astype(jnp.bfloat16)

        out_copy(r).start()

    spread(0)
    spread(1)
    for slot in range(WINDOW):
        key_at = (base_of(slot) + lane).astype(jnp.float32)
        seen = (key_at >= tokens_before) & (key_at <= row_at)
        bias[:, slot * ROWS : (slot + 1) * ROWS] = jnp.where(seen, 0.0, -1e30)
    for g in range(GROUPS):
        q_copy(g).wait()

    @pl.loop(0, GROUPS + 2)
    def _(i):
        @pl.when(i < GROUPS)
        def _():
            relay(i)

        @pl.when(i + 2 < GROUPS)
        def _():
            spread(i + 2)

        @pl.when(i >= 2)
        def _():
            attend(i - 2)

        @pl.when((i >= 1) & (i <= GROUPS))
        def _():
            gather(i - 1)

    @pl.loop(0, GROUPS)
    def _(r):
        for kind in (UP, TO_E, TO_W, REL_E, REL_W, D_X, D_W, D_E, D_O):
            copy(r, kind).wait_send()

        @pl.when(y == 0)
        def _():
            copy(r, LIFT_E).wait_send()
            copy(r, LIFT_K).wait_send()

        out_copy(r).wait()


def body(query, key, value, query_gain, key_gain, positions, doc_start):
    half = np.arange(HEAD // 2, dtype=np.float32)
    inv_freq = ROPE_BASE ** (-(jnp.asarray(half) * 2.0 / HEAD))
    freq = jnp.concatenate([inv_freq, inv_freq]).reshape(1, HEAD)
    nz = lax.axis_size("sp") // (2 * COLS)
    vmem = pl.BlockSpec(memory_space=pltpu.VMEM)
    anywhere = pl.BlockSpec(memory_space=pl.ANY)
    return pl.pallas_call(
        functools.partial(kernel, nz),
        out_shape=jax.ShapeDtypeStruct((ROWS, QUERY_HEADS * HEAD), jnp.bfloat16),
        in_specs=[anywhere, vmem, anywhere, vmem, vmem, vmem, vmem, vmem],
        out_specs=anywhere,
        scratch_shapes=[
            pltpu.VMEM((GROUPS, SLOTS, 2, ROWS, HEAD), jnp.bfloat16),
            pltpu.VMEM((GROUPS, ROWS, COPIES * HEAD), jnp.bfloat16),
            pltpu.VMEM((GROUPS, ROWS, COPIES * HEAD), jnp.bfloat16),
            pltpu.VMEM((ROWS, WINDOW * ROWS), jnp.float32),
            pltpu.VMEM((ROWS, HEAD), jnp.float32),
            pltpu.VMEM((ROWS, HEAD), jnp.float32),
            pltpu.SemaphoreType.DMA((GROUPS, KINDS)),
            pltpu.SemaphoreType.DMA((GROUPS, KINDS)),
            pltpu.SemaphoreType.DMA((GROUPS,)),
            pltpu.SemaphoreType.DMA((GROUPS,)),
            pltpu.SemaphoreType.DMA((GROUPS,)),
        ],
        compiler_params=pltpu.CompilerParams(
            collective_id=0, has_side_effects=True, vmem_limit_bytes=60 * 1024 * 1024
        ),
    )(
        query,
        key,
        value,
        query_gain.reshape(1, HEAD),
        key_gain.reshape(1, HEAD),
        positions.reshape(1, ROWS),
        doc_start.reshape(1, ROWS),
        freq,
    )


def solution(mesh):
    rows = P(("dp", "sp"), None)
    line = P(("dp", "sp"))
    return jax.shard_map(
        body,
        mesh=mesh,
        in_specs=(rows, rows, rows, P(), P(), line, line),
        out_specs=rows,
        check_vma=False,
    )
```

```python
import functools

import jax
import jax.numpy as jnp
import numpy as np
from jax import lax
from jax.experimental import pallas as pl
from jax.experimental.pallas import tpu as pltpu
from jax.sharding import PartitionSpec as P

QUERY_HEADS = 64
GROUPS = 8
HEAD = 128
COPIES = QUERY_HEADS // GROUPS
ROWS = 128
ROPE_BASE = 1000000.0
NORM_EPS = 1e-06
COLS = 4

OWN, PREV, WEST, EAST, OPP, X_P, WEST_P, EAST_P, OPP_P, HOLD_E, HOLD_K = range(11)
WINDOW = 9
SLOTS = 11
UP, TO_E, TO_W, REL_E, REL_W, LIFT_E, LIFT_K, D_X, D_W, D_E, D_O = range(11)
KINDS = 11
MESH = pl.DeviceIdType.MESH
HEADS_AT_ONCE = 2
STEPS = COPIES // HEADS_AT_ONCE


def kernel(
    nz,
    q_hbm,
    k_ref,
    v_hbm,
    q_gain_ref,
    k_gain_ref,
    pos_ref,
    doc_ref,
    freq_ref,
    out_hbm,
    kv,
    q_in,
    out_buf,
    bias,
    cos_tab,
    sin_tab,
    send_sem,
    recv_sem,
    q_sem,
    v_sem,
    out_sem,
):
    me = lax.axis_index("sp")
    core = lax.rem(me, 2)
    y = lax.rem(lax.div(me, 2), COLS)
    z = lax.div(me, 2 * COLS)

    def device(z_at, y_at, core_at):
        return (z_at * COLS + y_at) * 2 + core_at

    east_y = lax.rem(y + 1, COLS)
    west_y = lax.rem(y + COLS - 1, COLS)
    opp_y = lax.rem(y + 2, COLS)
    east = device(z, east_y, core)
    west = device(z, west_y, core)
    up = device(lax.rem(z + 1, nz), y, core)
    down = device(lax.rem(z + nz - 1, nz), y, core)
    partner = device(z, y, 1 - core)

    src_e = jnp.where(y == 3, PREV, OWN)
    src_w = jnp.where(y >= 2, PREV, OWN)
    dst_w = jnp.where(y == 1, HOLD_E, EAST)
    dst_rel_e = jnp.where(y == 3, HOLD_K, OPP)
    src_rel_w = jnp.where(y == 0, HOLD_E, EAST)
    src_x = jnp.where(core == 0, OWN, PREV)

    def copy(r, kind):
        src, dst, target = {
            UP: (kv.at[r, OWN], kv.at[r, PREV], up),
            TO_E: (kv.at[r, src_e], kv.at[r, WEST], east),
            TO_W: (kv.at[r, src_w], kv.at[r, dst_w], west),
            REL_E: (kv.at[r, WEST, 0], kv.at[r, dst_rel_e, 0], east),
            REL_W: (kv.at[r, src_rel_w, 1], kv.at[r, OPP, 1], west),
            LIFT_E: (kv.at[r, HOLD_E], kv.at[r, EAST], up),
            LIFT_K: (kv.at[r, HOLD_K, 0], kv.at[r, OPP, 0], up),
            D_X: (kv.at[r, src_x], kv.at[r, X_P], partner),
            D_W: (kv.at[r, WEST], kv.at[r, WEST_P], partner),
            D_E: (kv.at[r, EAST], kv.at[r, EAST_P], partner),
            D_O: (kv.at[r, OPP], kv.at[r, OPP_P], partner),
        }[kind]
        return pltpu.make_async_remote_copy(
            src_ref=src,
            dst_ref=dst,
            send_sem=send_sem.at[r, kind],
            recv_sem=recv_sem.at[r, kind],
            device_id={"sp": target},
            device_id_type=MESH,
        )

    def v_copy(g):
        return pltpu.make_async_copy(
            v_hbm.at[:, pl.ds(g * HEAD, HEAD)], kv.at[g, OWN, 1], v_sem.at[g]
        )

    def q_copy(g):
        return pltpu.make_async_copy(
            q_hbm.at[:, pl.ds(g * COPIES * HEAD, COPIES * HEAD)], q_in.at[g], q_sem.at[g]
        )

    def out_copy(g):
        return pltpu.make_async_copy(
            out_buf.at[g],
            out_hbm.at[:, pl.ds(pl.multiple_of(g * COPIES * HEAD, COPIES * HEAD), COPIES * HEAD)],
            out_sem.at[g],
        )

    barrier = pltpu.get_barrier_semaphore()
    for target in (east, west, up, down, partner):
        pl.semaphore_signal(barrier, inc=1, device_id={"sp": target}, device_id_type=MESH)
    for g in range(GROUPS):
        v_copy(g).start()
    for g in range(GROUPS):
        q_copy(g).start()

    def column(row):
        return jnp.transpose(jnp.broadcast_to(row.astype(jnp.float32), (ROWS, ROWS)))

    angle = column(pos_ref[...]) * freq_ref[...]
    lane = lax.broadcasted_iota(jnp.int32, (ROWS, HEAD), 1)
    cos_tab[...] = jnp.cos(angle)
    sine = jnp.sin(angle)
    sin_tab[...] = jnp.where(lane < HEAD // 2, -sine, sine)

    def norm_rope(block, gain):
        x = block.astype(jnp.float32)
        mean_square = jnp.mean(x * x, axis=1, keepdims=True)
        normed = x * lax.rsqrt(mean_square + NORM_EPS) * gain
        turned = pltpu.roll(normed, HEAD // 2, 1)
        return (normed * cos_tab[...] + turned * sin_tab[...]).astype(jnp.bfloat16)

    for g in range(GROUPS):
        kv[g, OWN, 0] = norm_rope(k_ref[:, g * HEAD : (g + 1) * HEAD], k_gain_ref[...])
    for g in range(GROUPS):
        v_copy(g).wait()
    pl.semaphore_wait(barrier, 5)

    @pl.loop(0, GROUPS)
    def _(r):
        copy(r, UP).start()

    def spread(r):
        copy(r, UP).wait_recv()
        copy(r, TO_E).start()
        copy(r, TO_W).start()
        copy(r, D_X).start()

    def relay(r):
        copy(r, TO_E).wait_recv()
        copy(r, REL_E).start()
        copy(r, D_W).start()
        copy(r, TO_W).wait_recv()
        copy(r, REL_W).start()

        @pl.when(y == 0)
        def _():
            copy(r, LIFT_E).start()

        @pl.when(y != 0)
        def _():
            copy(r, D_E).start()

    def gather_east(r):
        copy(r, REL_E).wait_recv()

        @pl.when(y == 0)
        def _():
            copy(r, LIFT_K).start()

    def gather_west(r):
        @pl.when(y == 0)
        def _():
            copy(r, LIFT_E).wait_recv()
            copy(r, D_E).start()
            copy(r, LIFT_K).wait_recv()

        copy(r, REL_W).wait_recv()
        copy(r, D_O).start()

    row_first = me * ROWS
    tokens_before = column(doc_ref[...])
    row_at = (row_first + lax.broadcasted_iota(jnp.int32, (ROWS, ROWS), 0)).astype(jnp.float32)

    def base_of(slot):
        if slot == OWN:
            return me * ROWS
        if slot == X_P:
            of_prev = device(z - 1, y, 1 - core)
            return jnp.where(core == 1, me - 1, of_prev) * ROWS
        col = {PREV: y, WEST: west_y, EAST: east_y, OPP: opp_y}[
            slot if slot < X_P else slot - X_P + PREV
        ]
        at = core if slot < X_P else 1 - core
        return device(jnp.where(col >= y, z - 1, z), col, at) * ROWS

    def attend(r, step):
        @pl.when(step == 0)
        def _():
            for kind in (D_X, D_W, D_E, D_O):
                copy(r, kind).wait_recv()

        keys = kv[r, pl.ds(0, WINDOW), 0].reshape(WINDOW * ROWS, HEAD)
        values = kv[r, pl.ds(0, WINDOW), 1].reshape(WINDOW * ROWS, HEAD)
        wide = HEADS_AT_ONCE * HEAD
        at = pl.multiple_of(step * wide, wide)
        block = q_in[r, :, pl.ds(at, wide)]
        for h in range(HEADS_AT_ONCE):
            q = norm_rope(block[:, h * HEAD : (h + 1) * HEAD], q_gain_ref[...])
            scores = lax.dot_general(
                q, keys, (((1,), (1,)), ((), ())), preferred_element_type=jnp.float32
            )
            scores = scores * HEAD ** (-0.5) + bias[...]
            top = jnp.max(scores, axis=1, keepdims=True)
            exp_scores = jnp.exp(scores - top)
            total = jnp.sum(exp_scores, axis=1, keepdims=True)
            mixed = jnp.dot(
                exp_scores.astype(jnp.bfloat16), values, preferred_element_type=jnp.float32
            )
            out_buf[r, :, pl.ds(pl.multiple_of(at + h * HEAD, HEAD), HEAD)] = (
                mixed / total
            ).astype(jnp.bfloat16)

        @pl.when(step == STEPS - 1)
        def _():
            out_copy(r).start()

    spread(0)
    spread(1)
    for slot in range(WINDOW):
        key_at = (base_of(slot) + lane).astype(jnp.float32)
        seen = (key_at >= tokens_before) & (key_at <= row_at)
        bias[:, slot * ROWS : (slot + 1) * ROWS] = jnp.where(seen, 0.0, -1e30)
    for g in range(GROUPS):
        q_copy(g).wait()

    @pl.loop(0, (GROUPS + 2) * STEPS)
    def _(t):
        i = lax.div(t, STEPS)
        step = lax.rem(t, STEPS)

        @pl.when((step == 0) & (i < GROUPS))
        def _():
            relay(i)

        @pl.when((step == 0) & (i + 2 < GROUPS))
        def _():
            spread(i + 2)

        @pl.when((step == 1) & (i >= 1) & (i <= GROUPS))
        def _():
            gather_east(i - 1)

        @pl.when((step == STEPS - 1) & (i >= 1) & (i <= GROUPS))
        def _():
            gather_west(i - 1)

        @pl.when(i >= 2)
        def _():
            attend(i - 2, step)

    @pl.loop(0, GROUPS)
    def _(r):
        for kind in (UP, TO_E, TO_W, REL_E, REL_W, D_X, D_W, D_E, D_O):
            copy(r, kind).wait_send()

        @pl.when(y == 0)
        def _():
            copy(r, LIFT_E).wait_send()
            copy(r, LIFT_K).wait_send()

        out_copy(r).wait()


def body(query, key, value, query_gain, key_gain, positions, doc_start):
    half = np.arange(HEAD // 2, dtype=np.float32)
    inv_freq = ROPE_BASE ** (-(jnp.asarray(half) * 2.0 / HEAD))
    freq = jnp.concatenate([inv_freq, inv_freq]).reshape(1, HEAD)
    nz = lax.axis_size("sp") // (2 * COLS)
    vmem = pl.BlockSpec(memory_space=pltpu.VMEM)
    anywhere = pl.BlockSpec(memory_space=pl.ANY)
    return pl.pallas_call(
        functools.partial(kernel, nz),
        out_shape=jax.ShapeDtypeStruct((ROWS, QUERY_HEADS * HEAD), jnp.bfloat16),
        in_specs=[anywhere, vmem, anywhere, vmem, vmem, vmem, vmem, vmem],
        out_specs=anywhere,
        scratch_shapes=[
            pltpu.VMEM((GROUPS, SLOTS, 2, ROWS, HEAD), jnp.bfloat16),
            pltpu.VMEM((GROUPS, ROWS, COPIES * HEAD), jnp.bfloat16),
            pltpu.VMEM((GROUPS, ROWS, COPIES * HEAD), jnp.bfloat16),
            pltpu.VMEM((ROWS, WINDOW * ROWS), jnp.float32),
            pltpu.VMEM((ROWS, HEAD), jnp.float32),
            pltpu.VMEM((ROWS, HEAD), jnp.float32),
            pltpu.SemaphoreType.DMA((GROUPS, KINDS)),
            pltpu.SemaphoreType.DMA((GROUPS, KINDS)),
            pltpu.SemaphoreType.DMA((GROUPS,)),
            pltpu.SemaphoreType.DMA((GROUPS,)),
            pltpu.SemaphoreType.DMA((GROUPS,)),
        ],
        compiler_params=pltpu.CompilerParams(
            collective_id=0, has_side_effects=True, vmem_limit_bytes=60 * 1024 * 1024
        ),
    )(
        query,
        key,
        value,
        query_gain.reshape(1, HEAD),
        key_gain.reshape(1, HEAD),
        positions.reshape(1, ROWS),
        doc_start.reshape(1, ROWS),
        freq,
    )


def solution(mesh):
    rows = P(("dp", "sp"), None)
    line = P(("dp", "sp"))
    return jax.shard_map(
        body,
        mesh=mesh,
        in_specs=(rows, rows, rows, P(), P(), line, line),
        out_specs=rows,
        check_vma=False,
    )
```

```python
import functools

import jax
import jax.numpy as jnp
import numpy as np
from jax import lax
from jax.experimental import pallas as pl
from jax.experimental.pallas import tpu as pltpu
from jax.sharding import PartitionSpec as P

QUERY_HEADS = 64
GROUPS = 8
HEAD = 128
COPIES = QUERY_HEADS // GROUPS
ROWS = 128
ROPE_BASE = 1000000.0
NORM_EPS = 1e-06
COLS = 4

OWN, PREV, WEST, EAST, OPP, X_P, WEST_P, EAST_P, OPP_P, HOLD_E, HOLD_K = range(11)
WINDOW = 9
SLOTS = 11
(UP, TO_EK, TO_EV, TO_WK, TO_WV, REL_E, REL_W, LIFT_E, LIFT_K, D_X, D_W, D_E, D_O) = range(13)
KINDS = 13
MESH = pl.DeviceIdType.MESH
LOOK = 2
PAIR = 2
STEPS = COPIES // PAIR
KEYS = WINDOW * ROWS
CHUNK = 32
EXP2_SCALE = HEAD**-0.5 * 1.4426950408889634


def kernel(
    nz,
    q_hbm,
    k_hbm,
    v_hbm,
    q_gain_ref,
    k_gain_ref,
    pos_ref,
    doc_ref,
    freq_ref,
    out_hbm,
    kv,
    k_in,
    q_in,
    q_rope,
    out_buf,
    bias,
    cos_tab,
    sin_tab,
    score_a,
    score_b,
    weight_a,
    weight_b,
    total_a,
    total_b,
    send_sem,
    recv_sem,
    q_sem,
    v_sem,
    k_sem,
    out_sem,
):
    me = lax.axis_index("sp")
    core = lax.rem(me, 2)
    y = lax.rem(lax.div(me, 2), COLS)
    z = lax.div(me, 2 * COLS)

    def device(z_at, y_at, core_at):
        return (z_at * COLS + y_at) * 2 + core_at

    east_y = lax.rem(y + 1, COLS)
    west_y = lax.rem(y + COLS - 1, COLS)
    opp_y = lax.rem(y + 2, COLS)
    east = device(z, east_y, core)
    west = device(z, west_y, core)
    up = device(jnp.minimum(z + 1, nz - 1), y, core)
    down = device(jnp.maximum(z - 1, 0), y, core)
    partner = device(z, y, 1 - core)

    has_up = z < nz - 1
    has_down = z > 0
    src_e = jnp.where((y == 3) & has_down, PREV, OWN)
    src_w = jnp.where((y >= 2) & has_down, PREV, OWN)
    dst_w = jnp.where(y == 1, HOLD_E, EAST)
    dst_rel_e = jnp.where(y == 3, HOLD_K, OPP)
    src_rel_w = jnp.where(y == 0, HOLD_E, EAST)
    src_x = jnp.where((core == 1) & has_down, PREV, OWN)
    lifts_up = (y == 0) & has_up
    lifted = (y == 0) & has_down

    def copy(r, kind):
        src, dst, target = {
            UP: (kv.at[r, OWN], kv.at[r, PREV], up),
            TO_EK: (kv.at[r, src_e, 0], kv.at[r, WEST, 0], east),
            TO_EV: (kv.at[r, src_e, 1], kv.at[r, WEST, 1], east),
            TO_WK: (kv.at[r, src_w, 0], kv.at[r, dst_w, 0], west),
            TO_WV: (kv.at[r, src_w, 1], kv.at[r, dst_w, 1], west),
            REL_E: (kv.at[r, WEST, 0], kv.at[r, dst_rel_e, 0], east),
            REL_W: (kv.at[r, src_rel_w, 1], kv.at[r, OPP, 1], west),
            LIFT_E: (kv.at[r, HOLD_E], kv.at[r, EAST], up),
            LIFT_K: (kv.at[r, HOLD_K, 0], kv.at[r, OPP, 0], up),
            D_X: (kv.at[r, src_x], kv.at[r, X_P], partner),
            D_W: (kv.at[r, WEST], kv.at[r, WEST_P], partner),
            D_E: (kv.at[r, EAST], kv.at[r, EAST_P], partner),
            D_O: (kv.at[r, OPP], kv.at[r, OPP_P], partner),
        }[kind]
        return pltpu.make_async_remote_copy(
            src_ref=src,
            dst_ref=dst,
            send_sem=send_sem.at[r, kind],
            recv_sem=recv_sem.at[r, kind],
            device_id={"sp": target},
            device_id_type=MESH,
        )

    def v_copy(g):
        return pltpu.make_async_copy(
            v_hbm.at[:, pl.ds(g * HEAD, HEAD)], kv.at[g, OWN, 1], v_sem.at[g]
        )

    def q_copy(g):
        return pltpu.make_async_copy(
            q_hbm.at[:, pl.ds(g * COPIES * HEAD, COPIES * HEAD)], q_in.at[g], q_sem.at[g]
        )

    def out_copy(g):
        return pltpu.make_async_copy(
            out_buf.at[g],
            out_hbm.at[:, pl.ds(pl.multiple_of(g * COPIES * HEAD, COPIES * HEAD), COPIES * HEAD)],
            out_sem.at[g],
        )

    barrier = pltpu.get_barrier_semaphore()

    def greet(target):
        pl.semaphore_signal(barrier, inc=1, device_id={"sp": target}, device_id_type=MESH)

    for target in (east, west, partner):
        greet(target)

    @pl.when(has_up)
    def _():
        greet(up)

    @pl.when(has_down)
    def _():
        greet(down)

    k_copy = pltpu.make_async_copy(k_hbm, k_in, k_sem)
    k_copy.start()
    for g in range(GROUPS):
        v_copy(g).start()
    for g in range(GROUPS):
        q_copy(g).start()

    def column(row):
        return jnp.transpose(jnp.broadcast_to(row.astype(jnp.float32), (ROWS, ROWS)))

    angle = column(pos_ref[...]) * freq_ref[...]
    lane = lax.broadcasted_iota(jnp.int32, (ROWS, HEAD), 1)
    cos_tab[...] = jnp.cos(angle)
    sine = jnp.sin(angle)
    sin_tab[...] = jnp.where(lane < HEAD // 2, -sine, sine)

    def norm_rope(block, gain):
        x = block.astype(jnp.float32)
        mean_square = jnp.mean(x * x, axis=1, keepdims=True)
        normed = x * lax.rsqrt(mean_square + NORM_EPS) * gain
        turned = pltpu.roll(normed, HEAD // 2, 1)
        return (normed * cos_tab[...] + turned * sin_tab[...]).astype(jnp.bfloat16)

    @pl.when(z == 0)
    def _():
        kv[:, PREV] = jnp.zeros((GROUPS, 2, ROWS, HEAD), jnp.bfloat16)

        @pl.when(y == 0)
        def _():
            kv[:, EAST] = jnp.zeros((GROUPS, 2, ROWS, HEAD), jnp.bfloat16)
            kv[:, OPP, 0] = jnp.zeros((GROUPS, ROWS, HEAD), jnp.bfloat16)

    k_copy.wait()
    for g in range(GROUPS):
        kv[g, OWN, 0] = norm_rope(k_in[:, g * HEAD : (g + 1) * HEAD], k_gain_ref[...])
    for g in range(GROUPS):
        v_copy(g).wait()
    pl.semaphore_wait(
        barrier, 3 + has_up.astype(jnp.int32) + has_down.astype(jnp.int32)
    )

    @pl.when(has_up)
    def _():
        @pl.loop(0, GROUPS)
        def _(r):
            copy(r, UP).start()

    def spread(r):
        @pl.when(has_down)
        def _():
            copy(r, UP).wait_recv()

        for kind in (TO_EK, TO_WV, TO_EV, TO_WK, D_X):
            copy(r, kind).start()

    def relay_first(r):
        copy(r, TO_EK).wait_recv()
        copy(r, REL_E).start()
        copy(r, TO_WV).wait_recv()
        copy(r, REL_W).start()

    def relay_second(r):
        copy(r, TO_EV).wait_recv()
        copy(r, D_W).start()
        copy(r, TO_WK).wait_recv()

        @pl.when(lifts_up)
        def _():
            copy(r, LIFT_E).start()

        @pl.when(y != 0)
        def _():
            copy(r, D_E).start()

    def gather_first(r):
        @pl.when(y == 0)
        def _():
            @pl.when(has_down)
            def _():
                copy(r, LIFT_E).wait_recv()

            copy(r, D_E).start()

        copy(r, REL_E).wait_recv()

        @pl.when(lifts_up)
        def _():
            copy(r, LIFT_K).start()

        copy(r, REL_W).wait_recv()

        @pl.when(y != 0)
        def _():
            copy(r, D_O).start()

    def gather_second(r):
        @pl.when(y == 0)
        def _():
            @pl.when(has_down)
            def _():
                copy(r, LIFT_K).wait_recv()

            copy(r, D_O).start()

    row_first = me * ROWS
    tokens_before = column(doc_ref[...])
    row_at = (row_first + lax.broadcasted_iota(jnp.int32, (ROWS, ROWS), 0)).astype(jnp.float32)

    def base_of(slot):
        if slot == OWN:
            return me * ROWS
        if slot == X_P:
            of_prev = device(z - 1, y, 1 - core)
            return jnp.where(core == 1, me - 1, of_prev) * ROWS
        col = {PREV: y, WEST: west_y, EAST: east_y, OPP: opp_y}[
            slot if slot < X_P else slot - X_P + PREV
        ]
        at = core if slot < X_P else 1 - core
        return device(jnp.where(col >= y, z - 1, z), col, at) * ROWS

    scores, weights, totals = (score_a, score_b), (weight_a, weight_b), (total_a, total_b)

    def arrive(r):
        for kind in (D_X, D_W, D_E, D_O):
            copy(r, kind).wait_recv()

    def score(r, step):
        keys = kv[r, pl.ds(0, WINDOW), 0].reshape(KEYS, HEAD)
        scores[step % 2][...] = lax.dot_general(
            q_rope[r, step], keys, (((1,), (1,)), ((), ())), preferred_element_type=jnp.float32
        )

    def weigh(step):
        for first in range(0, PAIR * ROWS, CHUNK):
            rows, at = pl.ds(first, CHUNK), first % ROWS
            part = scores[step % 2][rows, :] * EXP2_SCALE + bias[at : at + CHUNK, :]
            part = jnp.exp2(part - jnp.max(part, axis=1, keepdims=True))
            weights[step % 2][rows, :] = part.astype(jnp.bfloat16)
            total = part[:, :ROWS]
            for slot in range(1, WINDOW):
                total = total + part[:, slot * ROWS : (slot + 1) * ROWS]
            totals[step % 2][rows, :] = total

    def mix(r, step):
        values = kv[r, pl.ds(0, WINDOW), 1].reshape(KEYS, HEAD)
        mixed = jnp.dot(weights[step % 2][...], values, preferred_element_type=jnp.float32)
        mixed = mixed * (1.0 / jnp.sum(totals[step % 2][...], axis=1, keepdims=True))
        for h in range(PAIR):
            at = (step * PAIR + h) * HEAD
            out_buf[r, :, at : at + HEAD] = mixed[h * ROWS : (h + 1) * ROWS].astype(jnp.bfloat16)

    for r in range(LOOK):
        spread(r)
    for slot in range(WINDOW):
        key_at = (base_of(slot) + lane).astype(jnp.float32)
        seen = (key_at >= tokens_before) & (key_at <= row_at)
        bias[:, slot * ROWS : (slot + 1) * ROWS] = jnp.where(seen, 0.0, -1e30)

    @pl.loop(0, GROUPS)
    def _(g):
        q_copy(g).wait()
        for h in range(COPIES):
            q_rope[g, h // PAIR, (h % PAIR) * ROWS : (h % PAIR + 1) * ROWS] = norm_rope(
                q_in[g, :, h * HEAD : (h + 1) * HEAD], q_gain_ref[...]
            )

    @pl.loop(0, GROUPS + 2)
    def _(i):
        def at_step(step):
            if step == 0:

                @pl.when(i < GROUPS)
                def _():
                    relay_first(i)

                @pl.when(i + LOOK < GROUPS)
                def _():
                    spread(i + LOOK)

                @pl.when(i >= 2)
                def _():
                    gather_second(i - 2)

                @pl.when(i < GROUPS)
                def _():
                    relay_second(i)

                @pl.when(i >= 2)
                def _():
                    arrive(i - 2)

            if step == 2:

                @pl.when((i >= 1) & (i <= GROUPS))
                def _():
                    gather_first(i - 1)

        for step in range(STEPS):
            at_step(step)

            @pl.when(i >= 2)
            def _():
                score(i - 2, step)
                weigh(step - 1)
                late = jnp.maximum(i - 3, 0) if step < 2 else i - 2
                mix(late, (step - 2) % STEPS)
                if step == 1:

                    @pl.when(i >= 3)
                    def _():
                        out_copy(i - 3).start()

    weigh(STEPS - 1)
    mix(GROUPS - 1, STEPS - 2)
    mix(GROUPS - 1, STEPS - 1)
    out_copy(GROUPS - 1).start()

    @pl.loop(0, GROUPS)
    def _(r):
        for kind in (TO_EK, TO_EV, TO_WK, TO_WV, REL_E, REL_W, D_X, D_W, D_E, D_O):
            copy(r, kind).wait_send()

        @pl.when(has_up)
        def _():
            copy(r, UP).wait_send()

        @pl.when(lifts_up)
        def _():
            copy(r, LIFT_E).wait_send()
            copy(r, LIFT_K).wait_send()

        out_copy(r).wait()


def body(query, key, value, query_gain, key_gain, positions, doc_start):
    half = np.arange(HEAD // 2, dtype=np.float32)
    inv_freq = ROPE_BASE ** (-(jnp.asarray(half) * 2.0 / HEAD))
    freq = jnp.concatenate([inv_freq, inv_freq]).reshape(1, HEAD)
    nz = lax.axis_size("sp") // (2 * COLS)
    vmem = pl.BlockSpec(memory_space=pltpu.VMEM)
    anywhere = pl.BlockSpec(memory_space=pl.ANY)
    return pl.pallas_call(
        functools.partial(kernel, nz),
        out_shape=jax.ShapeDtypeStruct((ROWS, QUERY_HEADS * HEAD), jnp.bfloat16),
        in_specs=[anywhere, anywhere, anywhere, vmem, vmem, vmem, vmem, vmem],
        out_specs=anywhere,
        scratch_shapes=[
            pltpu.VMEM((GROUPS, SLOTS, 2, ROWS, HEAD), jnp.bfloat16),
            pltpu.VMEM((ROWS, GROUPS * HEAD), jnp.bfloat16),
            pltpu.VMEM((GROUPS, ROWS, COPIES * HEAD), jnp.bfloat16),
            pltpu.VMEM((GROUPS, STEPS, PAIR * ROWS, HEAD), jnp.bfloat16),
            pltpu.VMEM((GROUPS, ROWS, COPIES * HEAD), jnp.bfloat16),
            pltpu.VMEM((ROWS, KEYS), jnp.float32),
            pltpu.VMEM((ROWS, HEAD), jnp.float32),
            pltpu.VMEM((ROWS, HEAD), jnp.float32),
            pltpu.VMEM((PAIR * ROWS, KEYS), jnp.float32),
            pltpu.VMEM((PAIR * ROWS, KEYS), jnp.float32),
            pltpu.VMEM((PAIR * ROWS, KEYS), jnp.bfloat16),
            pltpu.VMEM((PAIR * ROWS, KEYS), jnp.bfloat16),
            pltpu.VMEM((PAIR * ROWS, ROWS), jnp.float32),
            pltpu.VMEM((PAIR * ROWS, ROWS), jnp.float32),
            pltpu.SemaphoreType.DMA((GROUPS, KINDS)),
            pltpu.SemaphoreType.DMA((GROUPS, KINDS)),
            pltpu.SemaphoreType.DMA((GROUPS,)),
            pltpu.SemaphoreType.DMA((GROUPS,)),
            pltpu.SemaphoreType.DMA,
            pltpu.SemaphoreType.DMA((GROUPS,)),
        ],
        compiler_params=pltpu.CompilerParams(
            collective_id=0, has_side_effects=True, vmem_limit_bytes=60 * 1024 * 1024
        ),
    )(
        query,
        key,
        value,
        query_gain.reshape(1, HEAD),
        key_gain.reshape(1, HEAD),
        positions.reshape(1, ROWS),
        doc_start.reshape(1, ROWS),
        freq,
    )


def solution(mesh):
    rows = P(("dp", "sp"), None)
    line = P(("dp", "sp"))
    return jax.shard_map(
        body,
        mesh=mesh,
        in_specs=(rows, rows, rows, P(), P(), line, line),
        out_specs=rows,
        check_vma=False,
    )
```

```python
import functools

import jax
import jax.numpy as jnp
import numpy as np
from jax import lax
from jax.experimental import pallas as pl
from jax.experimental.pallas import tpu as pltpu
from jax.sharding import PartitionSpec as P

QUERY_HEADS = 64
GROUPS = 8
HEAD = 128
COPIES = QUERY_HEADS // GROUPS
ROWS = 128
ROPE_BASE = 1000000.0
NORM_EPS = 1e-06
COLS = 4

OWN, PREV, WEST, EAST, OPP, X_P, WEST_P, EAST_P, OPP_P, HOLD_E, HOLD_K = range(11)
WINDOW = 9
SLOTS = 11
(UP, TO_EK, TO_EV, TO_WK, TO_WV, REL_E, REL_W, LIFT_E, LIFT_K, D_X, D_W, D_E, D_O) = range(13)
KINDS = 13
MESH = pl.DeviceIdType.MESH
LOOK = 2
PAIR = 2
STEPS = COPIES // PAIR
KEYS = WINDOW * ROWS
CHUNK = 32
FAR = 2.0**20
EXP2_SCALE = HEAD**-0.5 * 1.4426950408889634


def kernel(
    nz,
    q_hbm,
    k_hbm,
    v_hbm,
    q_gain_ref,
    k_gain_ref,
    pos_ref,
    doc_ref,
    freq_ref,
    out_ref,
    kv,
    k_in,
    q_in,
    q_rope,
    bias,
    cos_tab,
    sin_tab,
    q_mask,
    k_mask,
    *rest,
):
    scores, tops, weights, totals = (rest[4 * n : 4 * n + 4] for n in range(4))
    send_sem, recv_sem, q_sem, v_sem, k_sem = rest[16:]
    me = lax.axis_index("sp")
    core = lax.rem(me, 2)
    y = lax.rem(lax.div(me, 2), COLS)
    z = lax.div(me, 2 * COLS)

    def device(z_at, y_at, core_at):
        return (z_at * COLS + y_at) * 2 + core_at

    east_y = lax.rem(y + 1, COLS)
    west_y = lax.rem(y + COLS - 1, COLS)
    opp_y = lax.rem(y + 2, COLS)
    east = device(z, east_y, core)
    west = device(z, west_y, core)
    up = device(jnp.minimum(z + 1, nz - 1), y, core)
    down = device(jnp.maximum(z - 1, 0), y, core)
    partner = device(z, y, 1 - core)

    has_up = z < nz - 1
    has_down = z > 0
    src_e = jnp.where((y == 3) & has_down, PREV, OWN)
    src_w = jnp.where((y >= 2) & has_down, PREV, OWN)
    dst_w = jnp.where(y == 1, HOLD_E, EAST)
    dst_rel_e = jnp.where(y == 3, HOLD_K, OPP)
    src_rel_w = jnp.where(y == 0, HOLD_E, EAST)
    src_x = jnp.where((core == 1) & has_down, PREV, OWN)
    lifts_up = (y == 0) & has_up
    lifted = (y == 0) & has_down

    def copy(r, kind):
        src, dst, target = {
            UP: (kv.at[r, OWN], kv.at[r, PREV], up),
            TO_EK: (kv.at[r, src_e, 0], kv.at[r, WEST, 0], east),
            TO_EV: (kv.at[r, src_e, 1], kv.at[r, WEST, 1], east),
            TO_WK: (kv.at[r, src_w, 0], kv.at[r, dst_w, 0], west),
            TO_WV: (kv.at[r, src_w, 1], kv.at[r, dst_w, 1], west),
            REL_E: (kv.at[r, WEST, 0], kv.at[r, dst_rel_e, 0], east),
            REL_W: (kv.at[r, src_rel_w, 1], kv.at[r, OPP, 1], west),
            LIFT_E: (kv.at[r, HOLD_E], kv.at[r, EAST], up),
            LIFT_K: (kv.at[r, HOLD_K, 0], kv.at[r, OPP, 0], up),
            D_X: (kv.at[r, src_x], kv.at[r, X_P], partner),
            D_W: (kv.at[r, WEST], kv.at[r, WEST_P], partner),
            D_E: (kv.at[r, EAST], kv.at[r, EAST_P], partner),
            D_O: (kv.at[r, OPP], kv.at[r, OPP_P], partner),
        }[kind]
        return pltpu.make_async_remote_copy(
            src_ref=src,
            dst_ref=dst,
            send_sem=send_sem.at[r, kind],
            recv_sem=recv_sem.at[r, kind],
            device_id={"sp": target},
            device_id_type=MESH,
        )

    def v_copy(g):
        return pltpu.make_async_copy(
            v_hbm.at[:, pl.ds(g * HEAD, HEAD)], kv.at[g, OWN, 1], v_sem.at[g]
        )

    def q_copy(g):
        return pltpu.make_async_copy(
            q_hbm.at[:, pl.ds(pl.multiple_of(g * COPIES * HEAD, COPIES * HEAD), COPIES * HEAD)], q_in.at[g], q_sem.at[g]
        )

    barrier = pltpu.get_barrier_semaphore()

    def greet(target):
        pl.semaphore_signal(barrier, inc=1, device_id={"sp": target}, device_id_type=MESH)

    for target in (east, west, partner):
        greet(target)

    @pl.when(has_up)
    def _():
        greet(up)

    @pl.when(has_down)
    def _():
        greet(down)

    k_copy = pltpu.make_async_copy(k_hbm, k_in, k_sem)
    k_copy.start()
    for g in range(GROUPS):
        v_copy(g).start()
    for g in range(GROUPS):
        q_copy(g).start()

    def column(row):
        return jnp.transpose(jnp.broadcast_to(row.astype(jnp.float32), (ROWS, ROWS)))

    angle = column(pos_ref[...]) * freq_ref[...]
    lane = lax.broadcasted_iota(jnp.int32, (ROWS, HEAD), 1)
    cos_tab[...] = jnp.cos(angle)
    sine = jnp.sin(angle)
    sin_tab[...] = jnp.where(lane < HEAD // 2, -sine, sine)

    def norm_rope(block, gain):
        x = block.astype(jnp.float32)
        mean_square = jnp.mean(x * x, axis=1, keepdims=True)
        normed = x * lax.rsqrt(mean_square + NORM_EPS) * gain
        turned = pltpu.roll(normed, HEAD // 2, 1)
        return (normed * cos_tab[...] + turned * sin_tab[...]).astype(jnp.bfloat16)

    @pl.when(z == 0)
    def _():
        kv[:, PREV] = jnp.zeros((GROUPS, 2, ROWS, HEAD), jnp.bfloat16)

        @pl.when(y == 0)
        def _():
            kv[:, EAST] = jnp.zeros((GROUPS, 2, ROWS, HEAD), jnp.bfloat16)
            kv[:, OPP, 0] = jnp.zeros((GROUPS, ROWS, HEAD), jnp.bfloat16)

    k_copy.wait()
    for g in range(GROUPS):
        kv[g, OWN, 0] = norm_rope(k_in[:, g * HEAD : (g + 1) * HEAD], k_gain_ref[...])
    for g in range(GROUPS):
        v_copy(g).wait()
    pl.semaphore_wait(
        barrier, 3 + has_up.astype(jnp.int32) + has_down.astype(jnp.int32)
    )

    @pl.when(has_up)
    def _():
        @pl.loop(0, jnp.where(y == 0, LOOK, GROUPS))
        def _(r):
            copy(r, UP).start()

    def spread_own(r):
        @pl.when((z == 0) | (y < 3))
        def _():
            copy(r, TO_EK).start()
            copy(r, TO_EV).start()

        @pl.when((z == 0) | (y < 2))
        def _():
            copy(r, TO_WV).start()
            copy(r, TO_WK).start()

    def spread_above(r):
        @pl.when(y != 0)
        def _():
            @pl.when(has_down)
            def _():
                copy(r, UP).wait_recv()

                @pl.when(y == 3)
                def _():
                    copy(r, TO_EK).start()
                    copy(r, TO_EV).start()

                @pl.when(y >= 2)
                def _():
                    copy(r, TO_WV).start()
                    copy(r, TO_WK).start()

            copy(r, D_X).start()

    def relay_first(r):
        copy(r, TO_EK).wait_recv()
        copy(r, REL_E).start()
        copy(r, TO_WV).wait_recv()
        copy(r, REL_W).start()

    def relay_second(r):
        copy(r, TO_EV).wait_recv()
        copy(r, D_W).start()
        copy(r, TO_WK).wait_recv()

        @pl.when(lifts_up)
        def _():
            copy(r, LIFT_E).start()

        @pl.when(y != 0)
        def _():
            copy(r, D_E).start()

    def gather_first(r):
        copy(r, REL_E).wait_recv()

        @pl.when(lifts_up)
        def _():
            copy(r, LIFT_K).start()

            @pl.when(r + LOOK < GROUPS)
            def _():
                copy(r + LOOK, UP).start()

        copy(r, REL_W).wait_recv()

        @pl.when(y != 0)
        def _():
            copy(r, D_O).start()

        @pl.when(y == 0)
        def _():
            @pl.when(has_down)
            def _():
                copy(r, UP).wait_recv()

            copy(r, D_X).start()

            @pl.when(has_down)
            def _():
                copy(r, LIFT_E).wait_recv()

            copy(r, D_E).start()

    def gather_second(r):
        @pl.when(y == 0)
        def _():
            @pl.when(has_down)
            def _():
                copy(r, LIFT_K).wait_recv()

            copy(r, D_O).start()

    def finish_sends():
        @pl.loop(0, GROUPS)
        def _(r):
            for kind in (TO_EK, TO_EV, TO_WK, TO_WV, REL_E, REL_W, D_X, D_W, D_E, D_O):
                copy(r, kind).wait_send()

            @pl.when(has_up)
            def _():
                copy(r, UP).wait_send()

            @pl.when(lifts_up)
            def _():
                copy(r, LIFT_E).wait_send()
                copy(r, LIFT_K).wait_send()

    row_first = me * ROWS
    tokens_before = column(doc_ref[...])
    row_at = (row_first + lax.broadcasted_iota(jnp.int32, (ROWS, ROWS), 0)).astype(jnp.float32)

    def base_of(slot):
        if slot == OWN:
            return me * ROWS
        if slot == X_P:
            of_prev = device(z - 1, y, 1 - core)
            return jnp.where(core == 1, me - 1, of_prev) * ROWS
        col = {PREV: y, WEST: west_y, EAST: east_y, OPP: opp_y}[
            slot if slot < X_P else slot - X_P + PREV
        ]
        at = core if slot < X_P else 1 - core
        return device(jnp.where(col >= y, z - 1, z), col, at) * ROWS

    def arrive(r):
        for kind in (D_X, D_W, D_E, D_O):
            copy(r, kind).wait_recv()

    def score(r, step):
        keys = kv[r, pl.ds(0, WINDOW), 0].reshape(KEYS, HEAD)
        scores[step][...] = lax.dot_general(
            jnp.concatenate([q_rope[r, step], q_mask[...]], axis=1),
            jnp.concatenate([keys, k_mask[...]], axis=1),
            (((1,), (1,)), ((), ())),
            preferred_element_type=jnp.float32,
        )

    def chunks():
        for first in range(0, PAIR * ROWS, CHUNK):
            yield pl.ds(first, CHUNK), pl.ds(first % ROWS, CHUNK)

    def peak(step):
        for rows, own in chunks():
            top = scores[step][rows, :ROWS] + bias[own, :]
            for slot in range(1, WINDOW):
                top = jnp.maximum(top, scores[step][rows, slot * ROWS : (slot + 1) * ROWS])
            top = jnp.max(top, axis=1, keepdims=True) * EXP2_SCALE
            tops[step][rows, :] = jnp.broadcast_to(top, (CHUNK, ROWS))

    def weigh(step):
        for rows, own in chunks():
            top = tops[step][rows, :]
            total = None
            for slot in range(WINDOW):
                at = slice(slot * ROWS, (slot + 1) * ROWS)
                part = scores[step][rows, at]
                if slot == OWN:
                    part = part + bias[own, :]
                part = jnp.exp2(part * EXP2_SCALE - top)
                weights[step][rows, at] = part.astype(jnp.bfloat16)
                total = part if total is None else total + part
            totals[step][rows, :] = total

    def mix(r, step):
        values = kv[r, pl.ds(0, WINDOW), 1].reshape(KEYS, HEAD)
        mixed = jnp.dot(weights[step][...], values, preferred_element_type=jnp.float32)
        mixed = mixed * (1.0 / jnp.sum(totals[step][...], axis=1, keepdims=True))
        for h in range(PAIR):
            at = pl.multiple_of(r * COPIES * HEAD + (step * PAIR + h) * HEAD, HEAD)
            out_ref[:, pl.ds(at, HEAD)] = mixed[h * ROWS : (h + 1) * ROWS].astype(jnp.bfloat16)

    for r in range(LOOK):
        spread_own(r)
    key_row = lax.broadcasted_iota(jnp.int32, (ROWS, ROWS), 0)
    own_key = (row_first + lane).astype(jnp.float32)
    bias[...] = jnp.where((own_key >= tokens_before) & (own_key <= row_at), 0.0, -1e30)
    starts_here = jnp.where(tokens_before >= row_first.astype(jnp.float32), 1.0, 0.0)
    row_flags = jnp.where(lane == 0, 1.0, jnp.where(lane == 1, starts_here, 0.0))
    for h in range(PAIR):
        q_mask[h * ROWS : (h + 1) * ROWS] = row_flags.astype(jnp.bfloat16)
    k_mask[:ROWS] = jnp.zeros((ROWS, HEAD), jnp.bfloat16)
    for slot in range(1, WINDOW):
        key_at = (base_of(slot) + key_row).astype(jnp.float32)
        gone = jnp.where(key_at < tokens_before[:1], -FAR, 0.0)
        flags = jnp.where(lane == 0, gone, jnp.where(lane == 1, -FAR, 0.0))
        k_mask[slot * ROWS : (slot + 1) * ROWS] = flags.astype(jnp.bfloat16)

    def rope(g):
        q_copy(g).wait()
        for h in range(COPIES):
            q_rope[g, h // PAIR, (h % PAIR) * ROWS : (h % PAIR + 1) * ROWS] = norm_rope(
                q_in[g, :, h * HEAD : (h + 1) * HEAD], q_gain_ref[...]
            )

    @pl.loop(0, GROUPS // 2)
    def _(g):
        rope(g)

        @pl.when(g >= GROUPS // 2 - LOOK)
        def _():
            spread_above(g - (GROUPS // 2 - LOOK))

    def attend(r_score, step, r_mix):
        score(r_score, step)
        peak((step - 1) % STEPS)
        weigh((step - 2) % STEPS)
        mix(r_mix, (step - 3) % STEPS)

    @pl.loop(0, GROUPS + 2)
    def _(i):
        before = jnp.maximum(i - 3, 0)

        @pl.when(i < GROUPS)
        def _():
            relay_first(i)

        @pl.when(i + LOOK < GROUPS)
        def _():
            spread_own(i + LOOK)
            spread_above(i + LOOK)

        @pl.when(i < 2)
        def _():
            @pl.loop(0, 2)
            def _(n):
                rope(GROUPS // 2 + 2 * i + n)

        @pl.when(i >= 3)
        def _():
            attend(before, 2, jnp.maximum(i - 4, 0))

        @pl.when(i < GROUPS)
        def _():
            relay_second(i)

        @pl.when(i >= 3)
        def _():
            attend(before, 3, before)

        @pl.when((i >= 1) & (i <= GROUPS))
        def _():
            gather_first(i - 1)

        @pl.when(i >= 2)
        def _():
            gather_second(i - 2)

        @pl.when(i == GROUPS + 1)
        def _():
            finish_sends()

        @pl.when(i >= 2)
        def _():
            arrive(i - 2)
            attend(i - 2, 0, before)
            attend(i - 2, 1, before)

    last = GROUPS - 1
    attend(last, 2, last - 1)
    attend(last, 3, last)
    peak(3)
    weigh(2)
    mix(last, 1)
    weigh(3)
    mix(last, 2)
    mix(last, 3)


def body(query, key, value, query_gain, key_gain, positions, doc_start):
    half = np.arange(HEAD // 2, dtype=np.float32)
    inv_freq = ROPE_BASE ** (-(jnp.asarray(half) * 2.0 / HEAD))
    freq = jnp.concatenate([inv_freq, inv_freq]).reshape(1, HEAD)
    nz = lax.axis_size("sp") // (2 * COLS)
    vmem = pl.BlockSpec(memory_space=pltpu.VMEM)
    anywhere = pl.BlockSpec(memory_space=pltpu.HBM)
    return pl.pallas_call(
        functools.partial(kernel, nz),
        out_shape=pltpu.VMEM((ROWS, QUERY_HEADS * HEAD), jnp.bfloat16),
        in_specs=[anywhere, anywhere, anywhere, vmem, vmem, vmem, vmem, vmem],
        out_specs=vmem,
        scratch_shapes=[
            pltpu.VMEM((GROUPS, SLOTS, 2, ROWS, HEAD), jnp.bfloat16),
            pltpu.VMEM((ROWS, GROUPS * HEAD), jnp.bfloat16),
            pltpu.VMEM((GROUPS, ROWS, COPIES * HEAD), jnp.bfloat16),
            pltpu.VMEM((GROUPS, STEPS, PAIR * ROWS, HEAD), jnp.bfloat16),
            pltpu.VMEM((ROWS, ROWS), jnp.float32),
            pltpu.VMEM((ROWS, HEAD), jnp.float32),
            pltpu.VMEM((ROWS, HEAD), jnp.float32),
            pltpu.VMEM((PAIR * ROWS, HEAD), jnp.bfloat16),
            pltpu.VMEM((KEYS, HEAD), jnp.bfloat16),
            *[pltpu.VMEM((PAIR * ROWS, KEYS), jnp.float32)] * STEPS,
            *[pltpu.VMEM((PAIR * ROWS, ROWS), jnp.float32)] * STEPS,
            *[pltpu.VMEM((PAIR * ROWS, KEYS), jnp.bfloat16)] * STEPS,
            *[pltpu.VMEM((PAIR * ROWS, ROWS), jnp.float32)] * STEPS,
            pltpu.SemaphoreType.DMA((GROUPS, KINDS)),
            pltpu.SemaphoreType.DMA((GROUPS, KINDS)),
            pltpu.SemaphoreType.DMA((GROUPS,)),
            pltpu.SemaphoreType.DMA((GROUPS,)),
            pltpu.SemaphoreType.DMA,
        ],
        compiler_params=pltpu.CompilerParams(
            collective_id=0, has_side_effects=True, vmem_limit_bytes=60 * 1024 * 1024
        ),
    )(
        query,
        key,
        value,
        query_gain.reshape(1, HEAD),
        key_gain.reshape(1, HEAD),
        positions.reshape(1, ROWS),
        doc_start.reshape(1, ROWS),
        freq,
    )


def solution(mesh):
    rows = P(("dp", "sp"), None)
    line = P(("dp", "sp"))
    return jax.shard_map(
        body,
        mesh=mesh,
        in_specs=(rows, rows, rows, P(), P(), line, line),
        out_specs=rows,
        check_vma=False,
    )
```

```python
import functools

import jax
import jax.numpy as jnp
import numpy as np
from jax import lax
from jax.experimental import pallas as pl
from jax.experimental.pallas import tpu as pltpu
from jax.sharding import PartitionSpec as P

QUERY_HEADS = 64
GROUPS = 8
HEAD = 128
COPIES = QUERY_HEADS // GROUPS
ROWS = 128
ROPE_BASE = 1000000.0
NORM_EPS = 1e-06
COLS = 4

OWN, PREV, WEST, EAST, OPP, X_P, WEST_P, EAST_P, OPP_P, HOLD_E, HOLD_K = range(11)
WINDOW = 9
SLOTS = 11
(UP, TO_EK, TO_EV, TO_WK, TO_WV, REL_E, REL_W, LIFT_E, LIFT_K, D_X, D_W, D_E, D_O) = range(13)
KINDS = 13
MESH = pl.DeviceIdType.MESH
LOOK = 2
PAIR = 2
STEPS = COPIES // PAIR
KEYS = WINDOW * ROWS
CHUNK = 32
FAR = 2.0**20
EXP2_SCALE = HEAD**-0.5 * 1.4426950408889634


def kernel(
    nz,
    q_hbm,
    k_hbm,
    v_hbm,
    q_gain_ref,
    k_gain_ref,
    pos_ref,
    doc_ref,
    freq_ref,
    out_ref,
    kv,
    k_in,
    q_in,
    q_rope,
    bias,
    cos_tab,
    sin_tab,
    q_mask,
    k_mask,
    *rest,
):
    scores, tops, weights, totals = (rest[4 * n : 4 * n + 4] for n in range(4))
    send_sem, recv_sem, q_sem, v_sem, k_sem = rest[16:]
    me = lax.axis_index("sp")
    core = lax.rem(me, 2)
    y = lax.rem(lax.div(me, 2), COLS)
    z = lax.div(me, 2 * COLS)

    def device(z_at, y_at, core_at):
        return (z_at * COLS + y_at) * 2 + core_at

    east_y = lax.rem(y + 1, COLS)
    west_y = lax.rem(y + COLS - 1, COLS)
    opp_y = lax.rem(y + 2, COLS)
    east = device(z, east_y, core)
    west = device(z, west_y, core)
    up = device(jnp.minimum(z + 1, nz - 1), y, core)
    down = device(jnp.maximum(z - 1, 0), y, core)
    partner = device(z, y, 1 - core)

    has_up = z < nz - 1
    has_down = z > 0
    src_e = jnp.where((y == 3) & has_down, PREV, OWN)
    src_w = jnp.where((y >= 2) & has_down, PREV, OWN)
    dst_w = jnp.where(y == 1, HOLD_E, EAST)
    dst_rel_e = jnp.where(y == 3, HOLD_K, OPP)
    src_rel_w = jnp.where(y == 0, HOLD_E, EAST)
    src_x = jnp.where((core == 1) & has_down, PREV, OWN)
    lifts_up = (y == 0) & has_up
    lifted = (y == 0) & has_down

    def copy(r, kind):
        src, dst, target = {
            UP: (kv.at[r, OWN], kv.at[r, PREV], up),
            TO_EK: (kv.at[r, src_e, 0], kv.at[r, WEST, 0], east),
            TO_EV: (kv.at[r, src_e, 1], kv.at[r, WEST, 1], east),
            TO_WK: (kv.at[r, src_w, 0], kv.at[r, dst_w, 0], west),
            TO_WV: (kv.at[r, src_w, 1], kv.at[r, dst_w, 1], west),
            REL_E: (kv.at[r, WEST, 0], kv.at[r, dst_rel_e, 0], east),
            REL_W: (kv.at[r, src_rel_w, 1], kv.at[r, OPP, 1], west),
            LIFT_E: (kv.at[r, HOLD_E], kv.at[r, EAST], up),
            LIFT_K: (kv.at[r, HOLD_K, 0], kv.at[r, OPP, 0], up),
            D_X: (kv.at[r, src_x], kv.at[r, X_P], partner),
            D_W: (kv.at[r, WEST], kv.at[r, WEST_P], partner),
            D_E: (kv.at[r, EAST], kv.at[r, EAST_P], partner),
            D_O: (kv.at[r, OPP], kv.at[r, OPP_P], partner),
        }[kind]
        return pltpu.make_async_remote_copy(
            src_ref=src,
            dst_ref=dst,
            send_sem=send_sem.at[r, kind],
            recv_sem=recv_sem.at[r, kind],
            device_id={"sp": target},
            device_id_type=MESH,
        )

    def v_copy(g):
        return pltpu.make_async_copy(
            v_hbm.at[:, pl.ds(g * HEAD, HEAD)], kv.at[g, OWN, 1], v_sem.at[g]
        )

    def q_copy(g):
        return pltpu.make_async_copy(
            q_hbm.at[:, pl.ds(pl.multiple_of(g * COPIES * HEAD, COPIES * HEAD), COPIES * HEAD)], q_in.at[g], q_sem.at[g]
        )

    barrier = pltpu.get_barrier_semaphore()

    def greet(target):
        pl.semaphore_signal(barrier, inc=1, device_id={"sp": target}, device_id_type=MESH)

    for target in (east, west, partner):
        greet(target)

    @pl.when(has_up)
    def _():
        greet(up)

    @pl.when(has_down)
    def _():
        greet(down)

    k_copy = pltpu.make_async_copy(k_hbm, k_in, k_sem)
    k_copy.start()
    for g in range(GROUPS):
        v_copy(g).start()
    for g in range(GROUPS):
        q_copy(g).start()

    def column(row):
        return jnp.transpose(jnp.broadcast_to(row.astype(jnp.float32), (ROWS, ROWS)))

    angle = column(pos_ref[...]) * freq_ref[...]
    lane = lax.broadcasted_iota(jnp.int32, (ROWS, HEAD), 1)
    cos_tab[...] = jnp.cos(angle)
    sine = jnp.sin(angle)
    sin_tab[...] = jnp.where(lane < HEAD // 2, -sine, sine)

    def norm_rope(block, gain):
        x = block.astype(jnp.float32)
        mean_square = jnp.mean(x * x, axis=1, keepdims=True)
        normed = x * lax.rsqrt(mean_square + NORM_EPS) * gain
        turned = pltpu.roll(normed, HEAD // 2, 1)
        return (normed * cos_tab[...] + turned * sin_tab[...]).astype(jnp.bfloat16)

    @pl.when(z == 0)
    def _():
        kv[:, PREV] = jnp.zeros((GROUPS, 2, ROWS, HEAD), jnp.bfloat16)

        @pl.when(y == 0)
        def _():
            kv[:, EAST] = jnp.zeros((GROUPS, 2, ROWS, HEAD), jnp.bfloat16)
            kv[:, OPP, 0] = jnp.zeros((GROUPS, ROWS, HEAD), jnp.bfloat16)

    k_copy.wait()
    for g in range(GROUPS):
        kv[g, OWN, 0] = norm_rope(k_in[:, g * HEAD : (g + 1) * HEAD], k_gain_ref[...])
    for g in range(GROUPS):
        v_copy(g).wait()
    pl.semaphore_wait(
        barrier, 3 + has_up.astype(jnp.int32) + has_down.astype(jnp.int32)
    )

    @pl.when(has_up)
    def _():
        @pl.loop(0, jnp.where(y == 0, LOOK, GROUPS))
        def _(r):
            copy(r, UP).start()

    def spread_own(r):
        @pl.when((z == 0) | (y < 3))
        def _():
            copy(r, TO_EK).start()
            copy(r, TO_EV).start()

        @pl.when((z == 0) | (y < 2))
        def _():
            copy(r, TO_WV).start()
            copy(r, TO_WK).start()

    def spread_above(r):
        @pl.when(y != 0)
        def _():
            @pl.when(has_down)
            def _():
                copy(r, UP).wait_recv()

                @pl.when(y == 3)
                def _():
                    copy(r, TO_EK).start()
                    copy(r, TO_EV).start()

                @pl.when(y >= 2)
                def _():
                    copy(r, TO_WV).start()
                    copy(r, TO_WK).start()

            copy(r, D_X).start()

    def relay_first(r):
        copy(r, TO_EK).wait_recv()
        copy(r, REL_E).start()
        copy(r, TO_WV).wait_recv()
        copy(r, REL_W).start()

    def relay_second(r):
        copy(r, TO_EV).wait_recv()
        copy(r, D_W).start()
        copy(r, TO_WK).wait_recv()

        @pl.when(lifts_up)
        def _():
            copy(r, LIFT_E).start()

        @pl.when(y != 0)
        def _():
            copy(r, D_E).start()

    def gather_first(r):
        copy(r, REL_E).wait_recv()

        @pl.when(lifts_up)
        def _():
            copy(r, LIFT_K).start()

            @pl.when(r + LOOK < GROUPS)
            def _():
                copy(r + LOOK, UP).start()

        copy(r, REL_W).wait_recv()

        @pl.when(y != 0)
        def _():
            copy(r, D_O).start()

        @pl.when(y == 0)
        def _():
            @pl.when(has_down)
            def _():
                copy(r, UP).wait_recv()

            copy(r, D_X).start()

            @pl.when(has_down)
            def _():
                copy(r, LIFT_E).wait_recv()

            copy(r, D_E).start()

    def gather_second(r):
        @pl.when(y == 0)
        def _():
            @pl.when(has_down)
            def _():
                copy(r, LIFT_K).wait_recv()

            copy(r, D_O).start()

    def finish_sends():
        @pl.loop(0, GROUPS)
        def _(r):
            for kind in (TO_EK, TO_EV, TO_WK, TO_WV, REL_E, REL_W, D_X, D_W, D_E, D_O):
                copy(r, kind).wait_send()

            @pl.when(has_up)
            def _():
                copy(r, UP).wait_send()

            @pl.when(lifts_up)
            def _():
                copy(r, LIFT_E).wait_send()
                copy(r, LIFT_K).wait_send()

    row_first = me * ROWS
    tokens_before = column(doc_ref[...])
    row_at = (row_first + lax.broadcasted_iota(jnp.int32, (ROWS, ROWS), 0)).astype(jnp.float32)

    def base_of(slot):
        if slot == OWN:
            return me * ROWS
        if slot == X_P:
            of_prev = device(z - 1, y, 1 - core)
            return jnp.where(core == 1, me - 1, of_prev) * ROWS
        col = {PREV: y, WEST: west_y, EAST: east_y, OPP: opp_y}[
            slot if slot < X_P else slot - X_P + PREV
        ]
        at = core if slot < X_P else 1 - core
        return device(jnp.where(col >= y, z - 1, z), col, at) * ROWS

    def arrive(r):
        for kind in (D_X, D_W, D_E, D_O):
            copy(r, kind).wait_recv()

    def score(r, step):
        keys = kv[r, pl.ds(0, WINDOW), 0].reshape(KEYS, HEAD)
        scores[step][...] = lax.dot_general(
            jnp.concatenate([q_rope[r, step], q_mask[...]], axis=1),
            jnp.concatenate([keys, k_mask[...]], axis=1),
            (((1,), (1,)), ((), ())),
            preferred_element_type=jnp.float32,
        )

    def chunks():
        for first in range(0, PAIR * ROWS, CHUNK):
            yield pl.ds(first, CHUNK), pl.ds(first % ROWS, CHUNK)

    def peak(step):
        for rows, own in chunks():
            top = scores[step][rows, :ROWS] + bias[own, :]
            for slot in range(1, WINDOW):
                top = jnp.maximum(top, scores[step][rows, slot * ROWS : (slot + 1) * ROWS])
            top = jnp.max(top, axis=1, keepdims=True) * EXP2_SCALE
            tops[step][rows, :] = jnp.broadcast_to(top, (CHUNK, ROWS))

    def weigh(step):
        for rows, own in chunks():
            top = tops[step][rows, :]
            total = None
            for slot in range(WINDOW):
                at = slice(slot * ROWS, (slot + 1) * ROWS)
                part = scores[step][rows, at]
                if slot == OWN:
                    part = part + bias[own, :]
                part = jnp.exp2(part * EXP2_SCALE - top)
                weights[step][rows, at] = part.astype(jnp.bfloat16)
                total = part if total is None else total + part
            totals[step][rows, :] = total

    def mix(r, step):
        values = kv[r, pl.ds(0, WINDOW), 1].reshape(KEYS, HEAD)
        mixed = jnp.dot(weights[step][...], values, preferred_element_type=jnp.float32)
        mixed = mixed * (1.0 / jnp.sum(totals[step][...], axis=1, keepdims=True))
        for h in range(PAIR):
            at = pl.multiple_of(r * COPIES * HEAD + (step * PAIR + h) * HEAD, HEAD)
            out_ref[:, pl.ds(at, HEAD)] = mixed[h * ROWS : (h + 1) * ROWS].astype(jnp.bfloat16)

    for r in range(LOOK):
        spread_own(r)
    key_row = lax.broadcasted_iota(jnp.int32, (ROWS, ROWS), 0)
    own_key = (row_first + lane).astype(jnp.float32)
    bias[...] = jnp.where((own_key >= tokens_before) & (own_key <= row_at), 0.0, -1e30)
    starts_here = jnp.where(tokens_before >= row_first.astype(jnp.float32), 1.0, 0.0)
    row_flags = jnp.where(lane == 0, 1.0, jnp.where(lane == 1, starts_here, 0.0))
    for h in range(PAIR):
        q_mask[h * ROWS : (h + 1) * ROWS] = row_flags.astype(jnp.bfloat16)
    k_mask[:ROWS] = jnp.zeros((ROWS, HEAD), jnp.bfloat16)
    for slot in range(1, WINDOW):
        key_at = (base_of(slot) + key_row).astype(jnp.float32)
        gone = jnp.where(key_at < tokens_before[:1], -FAR, 0.0)
        flags = jnp.where(lane == 0, gone, jnp.where(lane == 1, -FAR, 0.0))
        k_mask[slot * ROWS : (slot + 1) * ROWS] = flags.astype(jnp.bfloat16)

    def rope(g):
        q_copy(g).wait()
        for h in range(COPIES):
            q_rope[g, h // PAIR, (h % PAIR) * ROWS : (h % PAIR + 1) * ROWS] = norm_rope(
                q_in[g, :, h * HEAD : (h + 1) * HEAD], q_gain_ref[...]
            )

    @pl.loop(0, GROUPS // 2)
    def _(g):
        rope(g)

        @pl.when(g >= GROUPS // 2 - LOOK)
        def _():
            spread_above(g - (GROUPS // 2 - LOOK))

    def attend(r_score, step, r_mix):
        score(r_score, step)
        peak((step - 1) % STEPS)
        weigh((step - 2) % STEPS)
        mix(r_mix, (step - 3) % STEPS)

    last = GROUPS - 1

    @pl.loop(0, GROUPS)
    def _(i):
        before = jnp.maximum(i - 3, 0)
        relay_first(i)

        @pl.when(i + LOOK < GROUPS)
        def _():
            spread_own(i + LOOK)
            spread_above(i + LOOK)

        @pl.when(i < 2)
        def _():
            @pl.loop(0, 2)
            def _(n):
                rope(GROUPS // 2 + 2 * i + n)

        @pl.when(i >= 3)
        def _():
            attend(before, 2, jnp.maximum(i - 4, 0))

        relay_second(i)

        @pl.when(i >= 3)
        def _():
            attend(before, 3, before)

        @pl.when(i >= 1)
        def _():
            gather_first(i - 1)

        @pl.when(i >= 2)
        def _():
            gather_second(i - 2)
            arrive(i - 2)
            attend(i - 2, 0, before)
            attend(i - 2, 1, before)

    attend(last - 2, 2, last - 3)
    attend(last - 2, 3, last - 2)
    gather_second(last - 1)
    arrive(last - 1)
    attend(last - 1, 0, last - 2)
    attend(last - 1, 1, last - 2)
    gather_first(last)
    attend(last - 1, 2, last - 2)
    attend(last - 1, 3, last - 1)
    peak(3)
    weigh(2)
    mix(last - 1, 1)
    weigh(3)
    mix(last - 1, 2)
    mix(last - 1, 3)
    gather_second(last)
    finish_sends()
    arrive(last)
    for step in range(STEPS + 3):
        if step < STEPS:
            score(last, step)
        if 1 <= step < STEPS + 1:
            peak(step - 1)
        if 2 <= step < STEPS + 2:
            weigh(step - 2)
        if step >= 3:
            mix(last, step - 3)


def body(query, key, value, query_gain, key_gain, positions, doc_start):
    inv_freq = ROPE_BASE ** (-np.arange(HEAD // 2) * 2.0 / HEAD)
    freq = np.concatenate([inv_freq, inv_freq]).astype(np.float32).reshape(1, HEAD)
    nz = lax.axis_size("sp") // (2 * COLS)
    vmem = pl.BlockSpec(memory_space=pltpu.VMEM)
    anywhere = pl.BlockSpec(memory_space=pltpu.HBM)
    return pl.pallas_call(
        functools.partial(kernel, nz),
        out_shape=pltpu.VMEM((ROWS, QUERY_HEADS * HEAD), jnp.bfloat16),
        in_specs=[anywhere, anywhere, anywhere, vmem, vmem, vmem, vmem, vmem],
        out_specs=vmem,
        scratch_shapes=[
            pltpu.VMEM((GROUPS, SLOTS, 2, ROWS, HEAD), jnp.bfloat16),
            pltpu.VMEM((ROWS, GROUPS * HEAD), jnp.bfloat16),
            pltpu.VMEM((GROUPS, ROWS, COPIES * HEAD), jnp.bfloat16),
            pltpu.VMEM((GROUPS, STEPS, PAIR * ROWS, HEAD), jnp.bfloat16),
            pltpu.VMEM((ROWS, ROWS), jnp.float32),
            pltpu.VMEM((ROWS, HEAD), jnp.float32),
            pltpu.VMEM((ROWS, HEAD), jnp.float32),
            pltpu.VMEM((PAIR * ROWS, HEAD), jnp.bfloat16),
            pltpu.VMEM((KEYS, HEAD), jnp.bfloat16),
            *[pltpu.VMEM((PAIR * ROWS, KEYS), jnp.float32)] * STEPS,
            *[pltpu.VMEM((PAIR * ROWS, ROWS), jnp.float32)] * STEPS,
            *[pltpu.VMEM((PAIR * ROWS, KEYS), jnp.bfloat16)] * STEPS,
            *[pltpu.VMEM((PAIR * ROWS, ROWS), jnp.float32)] * STEPS,
            pltpu.SemaphoreType.DMA((GROUPS, KINDS)),
            pltpu.SemaphoreType.DMA((GROUPS, KINDS)),
            pltpu.SemaphoreType.DMA((GROUPS,)),
            pltpu.SemaphoreType.DMA((GROUPS,)),
            pltpu.SemaphoreType.DMA,
        ],
        compiler_params=pltpu.CompilerParams(
            collective_id=0, has_side_effects=True, vmem_limit_bytes=60 * 1024 * 1024
        ),
    )(
        query,
        key,
        value,
        query_gain.reshape(1, HEAD),
        key_gain.reshape(1, HEAD),
        positions.reshape(1, ROWS),
        doc_start.reshape(1, ROWS),
        freq,
    )


def solution(mesh):
    rows = P(("dp", "sp"), None)
    line = P(("dp", "sp"))
    return jax.shard_map(
        body,
        mesh=mesh,
        in_specs=(rows, rows, rows, P(), P(), line, line),
        out_specs=rows,
        check_vma=False,
    )
```
